32 devices in a mesh: rows: 4 (over y, core), cols: 8 (over z, x), hub: 1.
Axes of the slice: x: 2, y: 2, z: 4, core: 2. Of those that a mesh axis runs over, the one named last changes fastest.
Arguments:
- light_bits: int32 [96, 3072], P('rows', 'cols'), may hold values from -2147483648 to 2147483647, as said below
- hub_bits: int32 [4, 3072], P('hub', 'cols'), may hold values from -2147483648 to 2147483647, as said below
- hub_ids: int32 [128], replicated, may hold values from 0 to 3071, as said below
Outputs:
- clustering: float32 [3072], P(('rows', 'cols'))
The draws below stay inside these ranges and needn't reach their ends.
Inputs may be any that keep to these rules, and one draw needn't show every extreme that they name: Every word holds 32 bits; the matrix of light_bits is symmetric with a zero diagonal. `hub_bits`: every word holds 32 bits. `hub_ids`: 128 distinct vertex numbers.
All inputs are finite; a program needn't handle non-finite values.
Results may differ from the reference program's by a relative error of at most 0.0003.
Values sent between devices are 32-bit elements; how exact they have to be, the bound alone decides.
A program may use at most 128 MiB of HBM per device.

```python
import jax
import jax.numpy as jnp
from jax import lax

VERTICES = 3072
HUBS = 128


def vertex_weights(key):
    vertex_rank = jax.random.permutation(jax.random.fold_in(key, 7), VERTICES).astype(jnp.int32)
    weight = 4 + 128 // (1 + vertex_rank // 32)
    return (vertex_rank, weight)


def pack_bits(linked):
    powers = jnp.left_shift(jnp.int32(1), jnp.arange(32, dtype=jnp.int32))
    grouped = linked.astype(jnp.int32).reshape(linked.shape[0] // 32, 32, linked.shape[1])
    return jnp.sum(grouped * powers[None, :, None], axis=1).astype(jnp.int32)


def draw_light_bits(key, part):
    vertex_rank, weight = vertex_weights(key)
    samples = jax.random.randint(jax.random.fold_in(key, 11), (VERTICES, VERTICES), 0, 8192, dtype=jnp.int32)
    linked = samples < weight[:, None] * weight[None, :]
    vertex_ids = jnp.arange(VERTICES, dtype=jnp.int32)
    one_side = jnp.logical_and(linked, vertex_ids[None, :] > vertex_ids[:, None])
    symmetric = jnp.logical_or(one_side, one_side.T)
    return pack_bits(symmetric)


def draw_hub_bits(key, part):
    vertex_rank, weight = vertex_weights(key)
    samples = jax.random.randint(jax.random.fold_in(key, 13), (HUBS, VERTICES), 0, 1024, dtype=jnp.int32)
    linked = samples < 48 + weight[None, :]
    return pack_bits(linked)


def draw_hub_ids(key, part):
    vertex_rank, weight = vertex_weights(key)
    by_rank = jnp.argsort(vertex_rank)
    return by_rank[:HUBS].astype(jnp.int32)


def setup_inputs(seed: int = 0) -> dict:
    streams_of = jax.random.split(jax.random.key(seed), 4)
    return {
        "light_bits": draw_light_bits(jax.random.fold_in(streams_of[3], 71), 0),
        "hub_bits": draw_hub_bits(jax.random.fold_in(streams_of[3], 71), 0),
        "hub_ids": draw_hub_ids(jax.random.fold_in(streams_of[3], 71), 0),
    }


def unpack(packed):
    shifts = jnp.arange(32, dtype=jnp.int32)
    bit_grid = jnp.bitwise_and(jnp.right_shift(packed[:, None, :], shifts[None, :, None]), 1)
    return bit_grid.reshape(packed.shape[0] * 32, packed.shape[1]).astype(jnp.float32)


def reference(light_bits, hub_bits, hub_ids):
    total = light_bits.shape[1]
    vertex_ids = jnp.arange(total, dtype=jnp.int32)
    is_hub = jnp.any(vertex_ids[:, None] == hub_ids[None, :], axis=1)
    light = jnp.where(is_hub, 0.0, 1.0).astype(jnp.float32)
    adjacency = unpack(light_bits) * light[:, None] * light[None, :]
    two_paths = jnp.dot(adjacency, adjacency, precision=lax.Precision.HIGHEST, preferred_element_type=jnp.float32)
    light_tri = 0.5 * jnp.sum(adjacency * two_paths, axis=1)
    hub_rows = unpack(hub_bits) * light[None, :]
    reach_hub = jnp.dot(hub_rows, adjacency, precision=lax.Precision.HIGHEST, preferred_element_type=jnp.float32)
    intersect = hub_rows * reach_hub
    hub_tri = 0.5 * jnp.sum(intersect, axis=1)
    hub_deg = jnp.sum(hub_rows, axis=1)
    owners = (vertex_ids[:, None] == hub_ids[None, :]).astype(jnp.float32)
    triangles = light_tri + jnp.sum(intersect, axis=0) + jnp.sum(owners * hub_tri[None, :], axis=1)
    degrees = jnp.sum(adjacency, axis=1) + jnp.sum(hub_rows, axis=0) + jnp.sum(owners * hub_deg[None, :], axis=1)
    return triangles / (1.0 + degrees)
```

```python
import functools

import jax
import jax.numpy as jnp
from jax import lax
from jax.experimental import pallas as pl
from jax.experimental.pallas import tpu as pltpu
from jax.sharding import PartitionSpec as P

LANES = 128
MESH = pl.DeviceIdType.MESH


def spread(row, value, other=0.0):
    masks = jnp.left_shift(jnp.int32(1), lax.broadcasted_iota(jnp.int32, (32, row.shape[1]), 0))
    return jnp.where((jnp.broadcast_to(row, masks.shape) & masks) != 0, value, other)


def kernel(
    R, C, G,
    light_hbm, hub_hbm, ids_ref, out_ref,
    rowbuf, colbuf, hubbuf, keep, hubcol, abuf, bbuf, acc, wsum, outbox, inbox,
    local_sem, row_send, row_recv, col_send, col_recv, hub_send, hub_recv, msg_send, msg_recv,
):
    r, c, g = lax.axis_index("rows"), lax.axis_index("cols"), lax.axis_index("hub")
    _, bw, bc = rowbuf.shape
    hw = hubbuf.shape[1]
    pc = bc // G
    q = C // R
    rows = 32 * bw
    nh = 32 * hw * G
    per = rows // C
    me = g * C + c

    own = [
        pltpu.make_async_copy(light_hbm, rowbuf.at[c], local_sem.at[0]),
        pltpu.make_async_copy(hub_hbm, hubbuf.at[me], local_sem.at[1]),
        pltpu.make_async_copy(light_hbm, colbuf.at[r], local_sem.at[2]),
    ]
    for copy in own:
        copy.start()

    def group_peer(d):
        slot = lax.rem(me + d, G * C)
        return slot, (r, lax.rem(slot, C), slot // C)

    def col_peer(d):
        slot = lax.rem(r + d, R)
        return slot, (slot, c, g)

    barrier = pltpu.get_barrier_semaphore()
    for d in range(1, G * C):
        pl.semaphore_signal(barrier, inc=1, device_id=group_peer(d)[1], device_id_type=MESH)
    for d in range(1, R):
        pl.semaphore_signal(barrier, inc=1, device_id=col_peer(d)[1], device_id_type=MESH)

    for copy in own:
        copy.wait()
    pl.semaphore_wait(barrier, G * C - 1 + R - 1)

    sends = []
    for d in range(1, C):
        to = lax.rem(c + d, C)
        sends.append(pltpu.make_async_remote_copy(
            src_ref=rowbuf.at[c], dst_ref=rowbuf.at[c], send_sem=row_send.at[d], recv_sem=row_recv.at[c],
            device_id=(r, to, g), device_id_type=MESH))
    for d in range(1, R):
        sends.append(pltpu.make_async_remote_copy(
            src_ref=colbuf.at[r], dst_ref=colbuf.at[r], send_sem=col_send.at[d], recv_sem=col_recv.at[r],
            device_id=col_peer(d)[1], device_id_type=MESH))
    for d in range(1, G * C):
        sends.append(pltpu.make_async_remote_copy(
            src_ref=hubbuf.at[me], dst_ref=hubbuf.at[me], send_sem=hub_send.at[d], recv_sem=hub_recv.at[me],
            device_id=group_peer(d)[1], device_id_type=MESH))
    for copy in sends:
        copy.start()

    for h in range(nh // LANES):
        hubcol[h * LANES:(h + 1) * LANES, :] = jnp.transpose(
            jnp.broadcast_to(ids_ref[h:h + 1, :], (LANES, LANES)))

    def hub_hits(base):
        return hubcol[...] == base + lax.broadcasted_iota(jnp.int32, (nh, LANES), 1)

    def light_lanes(t, carry):
        hit = jnp.max(jnp.where(hub_hits(t * LANES), 1, 0), axis=0, keepdims=True)
        keep[pl.ds(t, 1), :] = hit - 1
        return carry

    tiles = bc // LANES
    lax.fori_loop(0, C * tiles, light_lanes, 0)

    def keep_of(block):
        return jnp.concatenate([keep[pl.ds(block * tiles + t, 1), :] for t in range(tiles)], axis=1)

    bbuf[:, pc:] = jnp.full((bbuf.shape[0], LANES), 1.0, jnp.bfloat16)
    part = pl.ds(pl.multiple_of(g * pc, LANES), pc)
    acc[...] = jnp.zeros_like(acc)

    def step(s, carry):
        off = (s + 1) // 2 if isinstance(s, int) and s % 2 else None
        if isinstance(s, int):
            off = (s + 1) // 2 if s % 2 else R - s // 2
        else:
            off = lax.select(lax.rem(s, 2) == 1, (s + 1) // 2, R - s // 2)
        rk = lax.rem(c // q + off, R)

        @pl.when(rk != r)
        def _():
            pltpu.make_async_copy(colbuf.at[rk], colbuf.at[rk], col_recv.at[rk]).wait()

        for w in range(bw):
            bbuf[32 * w:32 * w + 32, :pc] = spread(colbuf[rk, w:w + 1, part], 1.0).astype(jnp.bfloat16)
        for k in range(q):
            ck = rk * q + k

            @pl.when(ck != c)
            def _():
                pltpu.make_async_copy(rowbuf.at[ck], rowbuf.at[ck], row_recv.at[ck]).wait()

            lanes = slice(k * bc, (k + 1) * bc)
            mask = keep_of(ck)
            for w in range(bw):
                abuf[32 * w:32 * w + 32, lanes] = spread(
                    rowbuf[ck, w:w + 1, :] & mask, 1.0).astype(jnp.bfloat16)
            for j in range(G):
                slot = j * C + ck

                @pl.when(slot != me)
                def _():
                    pltpu.make_async_copy(hubbuf.at[slot], hubbuf.at[slot], hub_recv.at[slot]).wait()

                for w in range(hw):
                    at = rows + 32 * (j * hw + w)
                    abuf[at:at + 32, lanes] = spread(
                        hubbuf[slot, w:w + 1, :] & mask, 1.0).astype(jnp.bfloat16)
        acc[...] += jnp.dot(abuf[...], bbuf[...], preferred_element_type=jnp.float32)
        return carry

    if R <= 4:
        for s in range(R):
            step(s, 0)
    else:
        lax.fori_loop(0, R, step, 0)

    for j in range(G):
        for w in range(hw):
            at = 32 * (j * hw + w)
            bbuf[at:at + 32, :pc] = spread(hubbuf[j * C + c, w:w + 1, part], 2.0).astype(jnp.bfloat16)
            for k in range(q):
                abuf[at:at + 32, k * bc:(k + 1) * bc] = spread(
                    hubbuf[j * C + r * q + k, w:w + 1, :], 1.0).astype(jnp.bfloat16)
    acc[:rows, :] += lax.dot_general(
        abuf[:nh, :], bbuf[:nh, :], (((0,), (0,)), ((), ())), preferred_element_type=jnp.float32)

    mask = jnp.concatenate(
        [keep[pl.ds(c * tiles + g * (pc // LANES) + t, 1), :] for t in range(pc // LANES)], axis=1)

    def close(row, at):
        hit = spread(row & mask, acc[at:at + 32, :pc])
        wsum[at:at + 32, :] = functools.reduce(
            jnp.add, [hit[:, t * LANES:(t + 1) * LANES] for t in range(pc // LANES)])

    for w in range(bw):
        close(rowbuf[c, w:w + 1, part], 32 * w)
    for j in range(G):
        for w in range(hw):
            close(hubbuf[j * C + c, w:w + 1, part], rows + 32 * (j * hw + w))

    hub_tri = jnp.sum(wsum[rows:, :], axis=1, keepdims=True)

    def partial(to):
        hits = hub_hits(r * rows + to * per)
        light = 1.0 - jnp.sum(jnp.where(hits, 1.0, 0.0), axis=0, keepdims=True)
        start = pl.multiple_of(to * per, 8)
        own_sum = jnp.sum(jnp.transpose(wsum[pl.ds(start, LANES), :]), axis=0, keepdims=True)
        return light * own_sum + jnp.sum(jnp.where(hits, hub_tri, 0.0), axis=0, keepdims=True)

    posts = []
    for d in range(1, G * C):
        slot, peer = group_peer(d)
        outbox[d] = partial(lax.rem(slot, C))
        post = pltpu.make_async_remote_copy(
            src_ref=outbox.at[d], dst_ref=inbox.at[me], send_sem=msg_send.at[d], recv_sem=msg_recv.at[me],
            device_id=peer, device_id_type=MESH)
        post.start()
        posts.append(post)

    tri = partial(c)
    hits = hub_hits(r * rows + c * per)
    light = 1.0 - jnp.sum(jnp.where(hits, 1.0, 0.0), axis=0, keepdims=True)
    start = pl.multiple_of(c * per, 8)
    deg = light * jnp.transpose(acc[pl.ds(start, LANES), pc:])[:1, :]
    deg = deg + jnp.sum(jnp.where(hits, acc[rows:, pc:], 0.0), axis=0, keepdims=True)
    for d in range(1, G * C):
        slot, _ = group_peer(d)
        pltpu.make_async_copy(inbox.at[slot], inbox.at[slot], msg_recv.at[slot]).wait()
        tri = tri + inbox[slot]
    out_ref[...] = (0.5 * tri / (1.0 + deg))[:, :per]
    for copy in sends + posts:
        copy.wait_send()


def body(light_bits, hub_bits, hub_ids):
    R, C, G = lax.axis_size("rows"), lax.axis_size("cols"), lax.axis_size("hub")
    bw, bc = light_bits.shape
    hw = hub_bits.shape[0]
    nh = hub_ids.shape[0]
    rows, pc = 32 * bw, bc // G
    per = rows // C
    dma = pltpu.SemaphoreType.DMA
    out = pl.pallas_call(
        functools.partial(kernel, R, C, G),
        out_shape=jax.ShapeDtypeStruct((1, per), jnp.float32),
        in_specs=[
            pl.BlockSpec(memory_space=pl.ANY),
            pl.BlockSpec(memory_space=pl.ANY),
            pl.BlockSpec(memory_space=pltpu.VMEM),
        ],
        out_specs=pl.BlockSpec(memory_space=pltpu.VMEM),
        scratch_shapes=[
            pltpu.VMEM((C, bw, bc), jnp.int32),
            pltpu.VMEM((R, bw, bc), jnp.int32),
            pltpu.VMEM((G * C, hw, bc), jnp.int32),
            pltpu.VMEM((C * bc // LANES, LANES), jnp.int32),
            pltpu.VMEM((nh, LANES), jnp.int32),
            pltpu.VMEM((rows + nh, rows), jnp.bfloat16),
            pltpu.VMEM((rows, pc + LANES), jnp.bfloat16),
            pltpu.VMEM((rows + nh, pc + LANES), jnp.float32),
            pltpu.VMEM((rows + nh, LANES), jnp.float32),
            pltpu.VMEM((G * C, 1, LANES), jnp.float32),
            pltpu.VMEM((G * C, 1, LANES), jnp.float32),
            dma((3,)), dma((C,)), dma((C,)), dma((R,)), dma((R,)),
            dma((G * C,)), dma((G * C,)), dma((G * C,)), dma((G * C,)),
        ],
        compiler_params=pltpu.CompilerParams(
            collective_id=0, has_side_effects=True, vmem_limit_bytes=56 * 1024 * 1024),
    )(light_bits, hub_bits, hub_ids.reshape(nh // LANES, LANES))
    return out.reshape(per)


def solution(mesh):
    return jax.shard_map(
        body,
        mesh=mesh,
        in_specs=(P("rows", "cols"), P("hub", "cols"), P()),
        out_specs=P(("rows", "cols")),
        check_vma=False,
    )
```

```python
import functools

import jax
import jax.numpy as jnp
from jax import lax
from jax.experimental import pallas as pl
from jax.experimental.pallas import tpu as pltpu
from jax.sharding import PartitionSpec as P

LANES = 128
MESH = pl.DeviceIdType.MESH


def spread(row, value, other=0.0):
    masks = jnp.left_shift(jnp.int32(1), lax.broadcasted_iota(jnp.int32, (32, row.shape[1]), 0))
    return jnp.where((jnp.broadcast_to(row, masks.shape) & masks) != 0, value, other)


def kernel(
    R, C, G,
    light_hbm, hub_hbm, ids_ref, out_ref,
    rowbuf, colbuf, hubbuf, keep, hubcol, abuf, bbuf, acc, wsum, outbox, inbox,
    local_sem, row_send, row_recv, col_send, col_recv, hub_send, hub_recv, msg_send, msg_recv,
):
    r, c, g = lax.axis_index("rows"), lax.axis_index("cols"), lax.axis_index("hub")
    _, bw, bc = rowbuf.shape
    hw = hubbuf.shape[1]
    pc = bc // G
    q = C // R
    rows = 32 * bw
    wq = bw // q
    nh = 32 * hw * G
    per = rows // C
    me = g * C + c

    own = [
        pltpu.make_async_copy(light_hbm, rowbuf.at[c], local_sem.at[0]),
        pltpu.make_async_copy(hub_hbm, hubbuf.at[me], local_sem.at[1]),
        pltpu.make_async_copy(light_hbm, colbuf.at[r], local_sem.at[2]),
    ]
    for copy in own:
        copy.start()

    def group_peer(d):
        slot = lax.rem(me + d, G * C)
        return slot, (r, lax.rem(slot, C), slot // C)

    def col_peer(d):
        slot = lax.rem(r + d, R)
        return slot, (slot, c, g)

    barrier = pltpu.get_barrier_semaphore()
    for d in range(1, G * C):
        pl.semaphore_signal(barrier, inc=1, device_id=group_peer(d)[1], device_id_type=MESH)
    for d in range(1, R):
        pl.semaphore_signal(barrier, inc=1, device_id=col_peer(d)[1], device_id_type=MESH)

    for copy in own:
        copy.wait()
    pl.semaphore_wait(barrier, G * C - 1 + R - 1)

    half = C // 2
    sends = []
    for d in range(half, 0, -1):
        sends.append(pltpu.make_async_remote_copy(
            src_ref=rowbuf.at[c], dst_ref=rowbuf.at[c], send_sem=row_send.at[d], recv_sem=row_recv.at[c],
            device_id=(r, lax.rem(c + C - d, C), g), device_id_type=MESH))
    for d in range(1, R):
        sends.append(pltpu.make_async_remote_copy(
            src_ref=colbuf.at[r], dst_ref=colbuf.at[r], send_sem=col_send.at[d], recv_sem=col_recv.at[r],
            device_id=col_peer(d)[1], device_id_type=MESH))
    for d in range(1, G * C):
        sends.append(pltpu.make_async_remote_copy(
            src_ref=hubbuf.at[me], dst_ref=hubbuf.at[me], send_sem=hub_send.at[d], recv_sem=hub_recv.at[me],
            device_id=group_peer(d)[1], device_id_type=MESH))
    for copy in sends:
        copy.start()

    for h in range(nh // LANES):
        hubcol[h * LANES:(h + 1) * LANES, :] = jnp.transpose(
            jnp.broadcast_to(ids_ref[h:h + 1, :], (LANES, LANES)))

    def hub_hits(base):
        return hubcol[...] == base + lax.broadcasted_iota(jnp.int32, (nh, LANES), 1)

    def light_lanes(t, carry):
        hit = jnp.max(jnp.where(hub_hits(t * LANES), 1, 0), axis=0, keepdims=True)
        keep[pl.ds(t, 1), :] = hit - 1
        return carry

    tiles = bc // LANES
    lax.fori_loop(0, C * tiles, light_lanes, 0)

    def keep_of(block):
        return jnp.concatenate([keep[pl.ds(block * tiles + t, 1), :] for t in range(tiles)], axis=1)

    part = pl.ds(pl.multiple_of(g * pc, LANES), pc)
    first = (g == 0).astype(jnp.float32)
    ones = jnp.full((bc, LANES), 1.0, jnp.float32)

    def load(d):
        ck = lax.rem(c + d, C)
        rk = ck // q
        base = d * bc
        weight = 1.0 if d == 0 or 2 * d == C else 2.0
        word0 = lax.rem(ck, q) * wq
        for w in range(wq):
            at = base + 32 * w
            bbuf[at:at + 32, :pc] = spread(colbuf[rk, pl.ds(word0 + w, 1), part], weight).astype(jnp.bfloat16)
        bbuf[base:base + bc, pc:] = (ones * (first if d == 0 else 0.0)).astype(jnp.bfloat16)
        mask = keep_of(ck)
        for w in range(bw):
            abuf[32 * w:32 * w + 32, base:base + bc] = spread(
                rowbuf[ck, w:w + 1, :] & mask, 1.0).astype(jnp.bfloat16)
        for j in range(G):
            for w in range(hw):
                at = rows + 32 * (j * hw + w)
                abuf[at:at + 32, base:base + bc] = spread(
                    hubbuf[j * C + ck, w:w + 1, :] & mask, 1.0).astype(jnp.bfloat16)

    for d in range(1, R):
        slot = col_peer(d)[0]
        pltpu.make_async_copy(colbuf.at[slot], colbuf.at[slot], col_recv.at[slot]).wait()
    load(0)
    for d in range(1, G * C):
        slot = group_peer(d)[0]
        pltpu.make_async_copy(hubbuf.at[slot], hubbuf.at[slot], hub_recv.at[slot]).wait()

    tail = (half + 1) * bc
    once = first * (c == 0).astype(jnp.float32)
    for j in range(G):
        for w in range(hw):
            at = tail + 32 * (j * hw + w)
            bbuf[at:at + 32, :pc] = spread(hubbuf[j * C + c, w:w + 1, part], 2.0).astype(jnp.bfloat16)
    bbuf[tail:, pc:] = jnp.broadcast_to(once, (nh, LANES)).astype(jnp.bfloat16)
    abuf[rows:, tail:] = jnp.zeros((nh, nh), jnp.bfloat16)
    for j in range(G):
        for k in range(q):
            bits = jnp.concatenate(
                [spread(hubbuf[j * C + r * q + k, w:w + 1, :], 1.0) for w in range(hw)], axis=0)
            lanes = slice(tail + 32 * hw * j, tail + 32 * hw * (j + 1))
            abuf[k * bc:(k + 1) * bc, lanes] = jnp.transpose(bits).astype(jnp.bfloat16)

    done = 0
    for d in range(1, half + 1):
        ck = lax.rem(c + d, C)
        pltpu.make_async_copy(rowbuf.at[ck], rowbuf.at[ck], row_recv.at[ck]).wait()
        load(d)
        if d % 2 or d == half:
            end = tail + nh if d == half else (d + 1) * bc
            part_sum = jnp.dot(abuf[:, done:end], bbuf[done:end, :], preferred_element_type=jnp.float32)
            acc[...] = part_sum if done == 0 else acc[...] + part_sum
            done = end

    mask = jnp.concatenate(
        [keep[pl.ds(c * tiles + g * (pc // LANES) + t, 1), :] for t in range(pc // LANES)], axis=1)

    def close(row, at):
        hit = spread(row & mask, acc[at:at + 32, :pc])
        wsum[at:at + 32, :] = functools.reduce(
            jnp.add, [hit[:, t * LANES:(t + 1) * LANES] for t in range(pc // LANES)])

    for w in range(bw):
        close(rowbuf[c, w:w + 1, part], 32 * w)
    for j in range(G):
        for w in range(hw):
            close(hubbuf[j * C + c, w:w + 1, part], rows + 32 * (j * hw + w))

    hub_tri = jnp.sum(wsum[rows:, :], axis=1, keepdims=True)

    def partial(to):
        hits = hub_hits(r * rows + to * per)
        light = 1.0 - jnp.sum(jnp.where(hits, 1.0, 0.0), axis=0, keepdims=True)
        start = pl.multiple_of(to * per, 8)
        own_sum = jnp.sum(jnp.transpose(wsum[pl.ds(start, LANES), :]), axis=0, keepdims=True)
        return light * own_sum + jnp.sum(jnp.where(hits, hub_tri, 0.0), axis=0, keepdims=True)

    def degrees(to):
        hits = hub_hits(r * rows + to * per)
        light = 1.0 - jnp.sum(jnp.where(hits, 1.0, 0.0), axis=0, keepdims=True)
        start = pl.multiple_of(to * per, 8)
        own_sum = jnp.transpose(acc[pl.ds(start, LANES), pc:])[:1, :]
        return light * own_sum + jnp.sum(jnp.where(hits, acc[rows:, pc:], 0.0), axis=0, keepdims=True)

    posts = []
    for d in range(1, G * C):
        slot, peer = group_peer(d)
        to = lax.rem(slot, C)
        outbox[d, 0:1, :] = partial(to)
        outbox[d, 1:2, :] = degrees(to)
        post = pltpu.make_async_remote_copy(
            src_ref=outbox.at[d], dst_ref=inbox.at[me], send_sem=msg_send.at[d], recv_sem=msg_recv.at[me],
            device_id=peer, device_id_type=MESH)
        post.start()
        posts.append(post)

    tri = partial(c)
    deg = degrees(c)
    for d in range(1, G * C):
        slot, _ = group_peer(d)
        pltpu.make_async_copy(inbox.at[slot], inbox.at[slot], msg_recv.at[slot]).wait()
        tri = tri + inbox[slot, 0:1, :]
        deg = deg + inbox[slot, 1:2, :]
    out_ref[...] = (0.5 * tri / (1.0 + deg))[:, :per]
    for copy in sends + posts:
        copy.wait_send()


def body(light_bits, hub_bits, hub_ids):
    R, C, G = lax.axis_size("rows"), lax.axis_size("cols"), lax.axis_size("hub")
    bw, bc = light_bits.shape
    hw = hub_bits.shape[0]
    nh = hub_ids.shape[0]
    rows, pc = 32 * bw, bc // G
    per = rows // C
    depth = (C // 2 + 1) * bc + nh
    dma = pltpu.SemaphoreType.DMA
    out = pl.pallas_call(
        functools.partial(kernel, R, C, G),
        out_shape=jax.ShapeDtypeStruct((1, per), jnp.float32),
        in_specs=[
            pl.BlockSpec(memory_space=pl.ANY),
            pl.BlockSpec(memory_space=pl.ANY),
            pl.BlockSpec(memory_space=pltpu.VMEM),
        ],
        out_specs=pl.BlockSpec(memory_space=pltpu.VMEM),
        scratch_shapes=[
            pltpu.VMEM((C, bw, bc), jnp.int32),
            pltpu.VMEM((R, bw, bc), jnp.int32),
            pltpu.VMEM((G * C, hw, bc), jnp.int32),
            pltpu.VMEM((C * bc // LANES, LANES), jnp.int32),
            pltpu.VMEM((nh, LANES), jnp.int32),
            pltpu.VMEM((rows + nh, depth), jnp.bfloat16),
            pltpu.VMEM((depth, pc + LANES), jnp.bfloat16),
            pltpu.VMEM((rows + nh, pc + LANES), jnp.float32),
            pltpu.VMEM((rows + nh, LANES), jnp.float32),
            pltpu.VMEM((G * C, 2, LANES), jnp.float32),
            pltpu.VMEM((G * C, 2, LANES), jnp.float32),
            dma((3,)), dma((C,)), dma((C,)), dma((R,)), dma((R,)),
            dma((G * C,)), dma((G * C,)), dma((G * C,)), dma((G * C,)),
        ],
        compiler_params=pltpu.CompilerParams(
            collective_id=0, has_side_effects=True, vmem_limit_bytes=56 * 1024 * 1024),
    )(light_bits, hub_bits, hub_ids.reshape(nh // LANES, LANES))
    return out.reshape(per)


def solution(mesh):
    return jax.shard_map(
        body,
        mesh=mesh,
        in_specs=(P("rows", "cols"), P("hub", "cols"), P()),
        out_specs=P(("rows", "cols")),
        check_vma=False,
    )
```

```python
import functools

import jax
import jax.numpy as jnp
from jax import lax
from jax.experimental import pallas as pl
from jax.experimental.pallas import tpu as pltpu
from jax.sharding import PartitionSpec as P

LANES = 128
MESH = pl.DeviceIdType.MESH


def spread(row, value, other=0.0):
    masks = jnp.left_shift(jnp.int32(1), lax.broadcasted_iota(jnp.int32, (32, row.shape[1]), 0))
    return jnp.where((jnp.broadcast_to(row, masks.shape) & masks) != 0, value, other)


def kernel(
    R, C, G,
    light_hbm, hub_hbm, ids_ref, out_ref,
    rowbuf, colbuf, hubbuf, keep, hubcol, abuf, bbuf, acc, wsum, outbox, inbox, flags,
    local_sem, row_send, row_recv, col_send, col_recv, hub_send, hub_recv, msg_send, msg_recv,
):
    r, c, g = lax.axis_index("rows"), lax.axis_index("cols"), lax.axis_index("hub")
    _, bw, bc = rowbuf.shape
    hw = hubbuf.shape[1]
    pc = bc // G
    q = C // R
    rows = 32 * bw
    wq = bw // q
    nh = 32 * hw * G
    per = rows // C
    me = g * C + c

    own = [
        pltpu.make_async_copy(light_hbm, rowbuf.at[c], local_sem.at[0]),
        pltpu.make_async_copy(hub_hbm, hubbuf.at[me], local_sem.at[1]),
        pltpu.make_async_copy(light_hbm, colbuf.at[r], local_sem.at[2]),
    ]
    for copy in own:
        copy.start()

    def group_peer(d):
        slot = lax.rem(me + d, G * C)
        return slot, (r, lax.rem(slot, C), slot // C)

    def col_peer(d):
        slot = lax.rem(r + d, R)
        return slot, (slot, c, g)

    barrier = pltpu.get_barrier_semaphore()
    for d in range(1, G * C):
        pl.semaphore_signal(barrier, inc=1, device_id=group_peer(d)[1], device_id_type=MESH)
    for d in range(1, R):
        pl.semaphore_signal(barrier, inc=1, device_id=col_peer(d)[1], device_id_type=MESH)

    for copy in own:
        copy.wait()
    pl.semaphore_wait(barrier, G * C - 1 + R - 1)

    half = C // 2
    home = c // q == r
    inner = jnp.logical_and(4 * c >= C, 4 * c < 3 * C)

    def hub_copy(dj, d):
        return pltpu.make_async_remote_copy(
            src_ref=hubbuf.at[me], dst_ref=hubbuf.at[me], send_sem=hub_send.at[dj * C + d],
            recv_sem=hub_recv.at[me], device_id_type=MESH,
            device_id=(r, lax.rem(c + C - d, C), lax.rem(g + G - dj, G)))

    hub_offsets = [(dj, d) for d in range(C - 1, -1, -1) for dj in range(G) if dj or d]

    def hub_moves(act):
        for dj, d in hub_offsets:
            if d <= half:
                act(dj, d)
            else:
                pl.when(home)(functools.partial(act, dj, d))

    hub_moves(lambda dj, d: hub_copy(dj, d).start())
    sends = []
    for d in range(half, 0, -1):
        sends.append(pltpu.make_async_remote_copy(
            src_ref=rowbuf.at[c], dst_ref=rowbuf.at[c], send_sem=row_send.at[d], recv_sem=row_recv.at[c],
            device_id=(r, lax.rem(c + C - d, C), g), device_id_type=MESH))
    for d in range(1, R):
        sends.append(pltpu.make_async_remote_copy(
            src_ref=colbuf.at[r], dst_ref=colbuf.at[r], send_sem=col_send.at[d], recv_sem=col_recv.at[r],
            device_id=col_peer(d)[1], device_id_type=MESH))
    pl.when(jnp.logical_not(inner))(sends[0].start)
    for copy in sends[1:]:
        copy.start()

    for h in range(nh // LANES):
        hubcol[h * LANES:(h + 1) * LANES, :] = jnp.transpose(
            jnp.broadcast_to(ids_ref[h:h + 1, :], (LANES, LANES)))

    def hub_hits(base):
        return hubcol[...] == base + lax.broadcasted_iota(jnp.int32, (nh, LANES), 1)

    def light_lanes(t, carry):
        hit = jnp.max(jnp.where(hub_hits(t * LANES), 1, 0), axis=0, keepdims=True)
        keep[pl.ds(t, 1), :] = hit - 1
        return carry

    tiles = bc // LANES
    lax.fori_loop(0, C * tiles, light_lanes, 0)

    def keep_of(block):
        return jnp.concatenate([keep[pl.ds(block * tiles + t, 1), :] for t in range(tiles)], axis=1)

    part = pl.ds(pl.multiple_of(g * pc, LANES), pc)
    first = (g == 0).astype(jnp.float32)
    ones = jnp.full((bc, LANES), 1.0, jnp.float32)

    def load(d):
        ck = lax.rem(c + d, C)
        rk = ck // q
        base = d * bc + (nh if d else 0)
        weight = 1.0 if d == 0 else 2.0
        word0 = lax.rem(ck, q) * wq
        for w in range(wq):
            at = base + 32 * w
            bbuf[at:at + 32, :pc] = spread(colbuf[rk, pl.ds(word0 + w, 1), part], weight).astype(jnp.bfloat16)
        if d == 0:
            bbuf[base:base + bc, pc:] = (ones * first).astype(jnp.bfloat16)
        mask = keep_of(ck)
        for w in range(bw):
            abuf[32 * w:32 * w + 32, base:base + bc] = spread(
                rowbuf[ck, w:w + 1, :] & mask, 1.0).astype(jnp.bfloat16)
        for j in range(G):
            for w in range(hw):
                at = rows + 32 * (j * hw + w)
                abuf[at:at + 32, base:base + bc] = spread(
                    hubbuf[j * C + ck, w:w + 1, :] & mask, 1.0).astype(jnp.bfloat16)

    for d in range(1, R):
        slot = col_peer(d)[0]
        pltpu.make_async_copy(colbuf.at[slot], colbuf.at[slot], col_recv.at[slot]).wait()
    load(0)

    def hub_wait(slot):
        pltpu.make_async_copy(hubbuf.at[slot], hubbuf.at[slot], hub_recv.at[slot]).wait()

    for dj, d in hub_offsets:
        ck = lax.rem(c + d, C)
        wait = functools.partial(hub_wait, lax.rem(g + dj, G) * C + ck)
        if d <= half:
            wait()
        else:
            pl.when(ck // q == r)(wait)

    once = first * (c == 0).astype(jnp.float32)
    for j in range(G):
        for w in range(hw):
            at = bc + 32 * (j * hw + w)
            bbuf[at:at + 32, :pc] = spread(hubbuf[j * C + c, w:w + 1, part], 2.0).astype(jnp.bfloat16)
    bbuf[bc:bc + nh, pc:] = jnp.broadcast_to(once, (nh, LANES)).astype(jnp.bfloat16)
    abuf[rows:, bc:bc + nh] = jnp.zeros((nh, nh), jnp.bfloat16)
    for j in range(G):
        for k in range(q):
            bits = jnp.concatenate(
                [spread(hubbuf[j * C + r * q + k, w:w + 1, :], 1.0) for w in range(hw)], axis=0)
            lanes = slice(bc + 32 * hw * j, bc + 32 * hw * (j + 1))
            abuf[k * bc:(k + 1) * bc, lanes] = jnp.transpose(bits).astype(jnp.bfloat16)
    done = bc + nh
    acc[...] = jnp.dot(abuf[:, :done], bbuf[:done, :], preferred_element_type=jnp.float32)

    def settle(to, d):
        hits = hub_hits(r * rows + to * per)
        light = 1.0 - jnp.sum(jnp.where(hits, 1.0, 0.0), axis=0, keepdims=True)
        start = pl.multiple_of(to * per, 8)
        own_sum = jnp.transpose(acc[pl.ds(start, LANES), pc:])[:1, :]
        outbox[d, 1:2, :] = light * own_sum + jnp.sum(
            jnp.where(hits, acc[rows:, pc:], 0.0), axis=0, keepdims=True)
        flags[d] = light

    for d in range(G * C):
        settle(lax.rem(group_peer(d)[0], C), d)

    def meet(d):
        ck = lax.rem(c + d, C)
        pltpu.make_async_copy(rowbuf.at[ck], rowbuf.at[ck], row_recv.at[ck]).wait()
        load(d)

    def add(begin, end):
        acc[:, :pc] += jnp.dot(abuf[:, begin:end], bbuf[begin:end, :pc], preferred_element_type=jnp.float32)

    for d in range(1, half):
        meet(d)
        if d % 2 == 0 or d == half - 1:
            add(done, (d + 1) * bc + nh)
            done = (d + 1) * bc + nh

    @pl.when(inner)
    def _():
        meet(half)
        add(done, (half + 1) * bc + nh)

    mask = jnp.concatenate(
        [keep[pl.ds(c * tiles + g * (pc // LANES) + t, 1), :] for t in range(pc // LANES)], axis=1)

    def close(row, at):
        hit = spread(row & mask, acc[at:at + 32, :pc])
        wsum[at:at + 32, :] = functools.reduce(
            jnp.add, [hit[:, t * LANES:(t + 1) * LANES] for t in range(pc // LANES)])

    for w in range(bw):
        close(rowbuf[c, w:w + 1, part], 32 * w)
    for j in range(G):
        for w in range(hw):
            close(hubbuf[j * C + c, w:w + 1, part], rows + 32 * (j * hw + w))

    hub_tri = jnp.sum(wsum[rows:, :], axis=1, keepdims=True)

    def partial(to, d):
        hits = hub_hits(r * rows + to * per)
        start = pl.multiple_of(to * per, 8)
        own_sum = jnp.sum(jnp.transpose(wsum[pl.ds(start, LANES), :]), axis=0, keepdims=True)
        return flags[d] * own_sum + jnp.sum(jnp.where(hits, hub_tri, 0.0), axis=0, keepdims=True)

    posts = []
    for d in sorted(range(1, G * C), key=lambda d: abs(2 * d - G * C)):
        slot, peer = group_peer(d)
        outbox[d, 0:1, :] = partial(lax.rem(slot, C), d)
        post = pltpu.make_async_remote_copy(
            src_ref=outbox.at[d], dst_ref=inbox.at[me], send_sem=msg_send.at[d], recv_sem=msg_recv.at[me],
            device_id=peer, device_id_type=MESH)
        post.start()
        posts.append(post)

    tri = partial(c, 0)
    deg = outbox[0, 1:2, :]
    for d in range(1, G * C):
        slot, _ = group_peer(d)
        pltpu.make_async_copy(inbox.at[slot], inbox.at[slot], msg_recv.at[slot]).wait()
        tri = tri + inbox[slot, 0:1, :]
        deg = deg + inbox[slot, 1:2, :]
    out_ref[...] = (0.5 * tri / (1.0 + deg))[:, :per]
    hub_moves(lambda dj, d: hub_copy(dj, d).wait_send())
    pl.when(jnp.logical_not(inner))(sends[0].wait_send)
    for copy in sends[1:] + posts:
        copy.wait_send()


def body(light_bits, hub_bits, hub_ids):
    R, C, G = lax.axis_size("rows"), lax.axis_size("cols"), lax.axis_size("hub")
    bw, bc = light_bits.shape
    hw = hub_bits.shape[0]
    nh = hub_ids.shape[0]
    rows, pc = 32 * bw, bc // G
    per = rows // C
    depth = (C // 2 + 1) * bc + nh
    dma = pltpu.SemaphoreType.DMA
    out = pl.pallas_call(
        functools.partial(kernel, R, C, G),
        out_shape=jax.ShapeDtypeStruct((1, per), jnp.float32),
        in_specs=[
            pl.BlockSpec(memory_space=pl.ANY),
            pl.BlockSpec(memory_space=pl.ANY),
            pl.BlockSpec(memory_space=pltpu.VMEM),
        ],
        out_specs=pl.BlockSpec(memory_space=pltpu.VMEM),
        scratch_shapes=[
            pltpu.VMEM((C, bw, bc), jnp.int32),
            pltpu.VMEM((R, bw, bc), jnp.int32),
            pltpu.VMEM((G * C, hw, bc), jnp.int32),
            pltpu.VMEM((C * bc // LANES, LANES), jnp.int32),
            pltpu.VMEM((nh, LANES), jnp.int32),
            pltpu.VMEM((rows + nh, depth), jnp.bfloat16),
            pltpu.VMEM((depth, pc + LANES), jnp.bfloat16),
            pltpu.VMEM((rows + nh, pc + LANES), jnp.float32),
            pltpu.VMEM((rows + nh, LANES), jnp.float32),
            pltpu.VMEM((G * C, 2, LANES), jnp.float32),
            pltpu.VMEM((G * C, 2, LANES), jnp.float32),
            pltpu.VMEM((G * C, 1, LANES), jnp.float32),
            dma((3,)), dma((C,)), dma((C,)), dma((R,)), dma((R,)),
            dma((G * C,)), dma((G * C,)), dma((G * C,)), dma((G * C,)),
        ],
        compiler_params=pltpu.CompilerParams(
            collective_id=0, has_side_effects=True, vmem_limit_bytes=56 * 1024 * 1024),
    )(light_bits, hub_bits, hub_ids.reshape(nh // LANES, LANES))
    return out.reshape(per)


def solution(mesh):
    return jax.shard_map(
        body,
        mesh=mesh,
        in_specs=(P("rows", "cols"), P("hub", "cols"), P()),
        out_specs=P(("rows", "cols")),
        check_vma=False,
    )
```
